8 devices in a mesh: dp: 1 (over z), tp: 2 (over y), kvp: 4 (over x, core).
Axes of the slice: x: 2, y: 2, z: 1, core: 2. Of those that a mesh axis runs over, the one named last changes fastest.
Arguments:
- x_in: bfloat16 [32, 3072], P('dp')
- ctx_len: int32 [32], P('dp')
- g_attn: bfloat16 [3072], replicated
- g_mlp: bfloat16 [3072], replicated
- w_qkv: bfloat16 [3072, 5120], P(None, 'tp')
- w_o: bfloat16 [3072, 3072], P(('tp', 'kvp'))
- w_gate: bfloat16 [3072, 8192], P(None, ('tp', 'kvp'))
- w_up: bfloat16 [3072, 8192], P(None, ('tp', 'kvp'))
- w_down: bfloat16 [8192, 3072], P(('tp', 'kvp'))
- k_cache: bfloat16 [32, 1024, 8, 128], P('dp', 'kvp', 'tp')
- v_cache: bfloat16 [32, 1024, 8, 128], P('dp', 'kvp', 'tp')
Outputs:
- output 1: bfloat16 [32, 3072], P('dp')
- output 2: bfloat16 [32, 1024, 8, 128], P('dp', 'kvp', 'tp')
- output 3: bfloat16 [32, 1024, 8, 128], P('dp', 'kvp', 'tp')
All inputs are finite; a program needn't handle non-finite values.
Results may differ from the reference program's by a relative error of at most 0.00825897.
Values sent between devices are 32-bit elements.
A program may use at most 1 GiB of HBM per device.

```python
import jax
import jax.numpy as jnp
from jax import lax

D = 3072
HEADS = 24
KV_HEADS = 8
HEAD = 128
FF = 8192
BATCH = 32
SEQ = 1024
NSEG = 16
GROUP = HEADS // KV_HEADS
ROPE_THETA = 500000.0
EPS = 1e-5
NEG_FILL = -1e30


def rms_norm(values, gain_vec):
    x_f32 = values.astype(jnp.float32)
    inv_rms = lax.rsqrt(jnp.mean(x_f32 * x_f32, axis=-1, keepdims=True) + EPS)
    return (x_f32 * inv_rms * gain_vec.astype(jnp.float32)).astype(jnp.bfloat16)


def rope_tables(ctx_len):
    inv_freq = ROPE_THETA ** (-2.0 * jnp.arange(HEAD // 2, dtype=jnp.float32) / HEAD)
    angles = ctx_len.astype(jnp.float32)[:, None] * inv_freq[None, :]
    return jnp.cos(angles), jnp.sin(angles)


def rotary(vectors, cos_t, sin_t):
    half_dim = vectors.shape[-1] // 2
    first_half = vectors[..., :half_dim]
    second_half = vectors[..., half_dim:]
    return jnp.concatenate([first_half * cos_t - second_half * sin_t, second_half * cos_t + first_half * sin_t], axis=-1)


def setup_inputs(seed: int = 0, part: int = 0) -> dict:
    root_key = jax.random.key(seed)
    shared_keys = jax.random.split(root_key, 7)
    part_keys = jax.random.split(jax.random.fold_in(root_key, part), 7)
    x_in = jax.random.normal(part_keys[0], (BATCH, D), jnp.float32).astype(jnp.bfloat16)
    ctx_len = jax.random.randint(part_keys[1], (BATCH,), SEQ // 4, SEQ, dtype=jnp.int32)
    full_row = jax.random.randint(part_keys[2], (), 0, BATCH, dtype=jnp.int32)
    ctx_len = jnp.where(jnp.arange(BATCH) == full_row, SEQ - 1, ctx_len).astype(jnp.int32)
    g_attn = (1.0 + 0.3 * jax.random.normal(shared_keys[0], (D,), jnp.float32)).astype(jnp.bfloat16)
    g_mlp = (1.0 + 0.3 * jax.random.normal(shared_keys[1], (D,), jnp.float32)).astype(jnp.bfloat16)
    w_qkv = (jax.random.normal(shared_keys[2], (D, KV_HEADS * (GROUP + 2) * HEAD), jnp.float32) * D ** -0.5).astype(jnp.bfloat16)
    w_o = (jax.random.normal(shared_keys[3], (HEADS * HEAD, D), jnp.float32) * (HEADS * HEAD) ** -0.5).astype(jnp.bfloat16)
    w_gate = (jax.random.normal(shared_keys[4], (D, FF), jnp.float32) * D ** -0.5).astype(jnp.bfloat16)
    w_up = (jax.random.normal(shared_keys[5], (D, FF), jnp.float32) * D ** -0.5).astype(jnp.bfloat16)
    w_down = (jax.random.normal(shared_keys[6], (FF, D), jnp.float32) * FF ** -0.5).astype(jnp.bfloat16)
    seg_shape = (BATCH, NSEG, 1, KV_HEADS, HEAD)
    noise_shape = (BATCH, NSEG, SEQ // NSEG, KV_HEADS, HEAD)
    cache_shape = (BATCH, SEQ, KV_HEADS, HEAD)
    k_cache = (jax.random.normal(part_keys[3], noise_shape, jnp.float32) + 0.5 * jax.random.normal(part_keys[4], seg_shape, jnp.float32)).reshape(cache_shape).astype(jnp.bfloat16)
    v_cache = (0.5 * jax.random.normal(part_keys[5], noise_shape, jnp.float32) + 2.0 * jax.random.normal(part_keys[6], seg_shape, jnp.float32)).reshape(cache_shape).astype(jnp.bfloat16)
    return {"x_in": x_in, "ctx_len": ctx_len, "g_attn": g_attn, "g_mlp": g_mlp, "w_qkv": w_qkv, "w_o": w_o, "w_gate": w_gate, "w_up": w_up, "w_down": w_down, "k_cache": k_cache, "v_cache": v_cache}


def reference(x_in, ctx_len, g_attn, g_mlp, w_qkv, w_o, w_gate, w_up, w_down, k_cache, v_cache):
    normed = rms_norm(x_in, g_attn)
    qkv_all = jnp.dot(normed, w_qkv, preferred_element_type=jnp.float32).reshape(BATCH, KV_HEADS, GROUP + 2, HEAD)
    cos_t, sin_t = rope_tables(ctx_len)
    queries = rotary(qkv_all[:, :, :GROUP], cos_t[:, None, None, :], sin_t[:, None, None, :]).astype(jnp.bfloat16)
    key_new = rotary(qkv_all[:, :, GROUP], cos_t[:, None, :], sin_t[:, None, :]).astype(jnp.bfloat16)
    val_new = qkv_all[:, :, GROUP + 1].astype(jnp.bfloat16)
    positions = jnp.arange(SEQ)
    hit_mask = (positions[None, :] == ctx_len[:, None])[:, :, None, None]
    k_out = jnp.where(hit_mask, key_new[:, None], k_cache)
    v_out = jnp.where(hit_mask, val_new[:, None], v_cache)
    score_scale = HEAD ** -0.5

    def one_request(row_args):
        q_row, k_row, v_row, length = row_args
        scores = jnp.einsum("grd,tgd->grt", q_row.astype(jnp.float32), k_row.astype(jnp.float32)) * score_scale
        scores = jnp.where(positions <= length, scores, NEG_FILL)
        row_max = jnp.max(scores, axis=-1, keepdims=True)
        prob_w = jnp.exp(scores - row_max)
        denom_sum = jnp.sum(prob_w, axis=-1)
        numer_acc = jnp.einsum("grt,tgd->grd", prob_w.astype(jnp.bfloat16).astype(jnp.float32), v_row.astype(jnp.float32))
        return (numer_acc / denom_sum[..., None]).reshape(HEADS * HEAD)

    attn_all = lax.map(one_request, (queries, k_out, v_out, ctx_len)).astype(jnp.bfloat16)
    hidden = (x_in.astype(jnp.float32) + jnp.dot(attn_all, w_o, preferred_element_type=jnp.float32)).astype(jnp.bfloat16)
    normed_mlp = rms_norm(hidden, g_mlp)
    gate_pre = jnp.dot(normed_mlp, w_gate, preferred_element_type=jnp.float32)
    up_proj = jnp.dot(normed_mlp, w_up, preferred_element_type=jnp.float32)
    act_out = (jax.nn.silu(gate_pre) * up_proj).astype(jnp.bfloat16)
    x_out = (hidden.astype(jnp.float32) + jnp.dot(act_out, w_down, preferred_element_type=jnp.float32)).astype(jnp.bfloat16)
    return (x_out, k_out, v_out)
```

```python
import functools

import jax
import jax.numpy as jnp
import numpy as np
from jax import lax
from jax.experimental import pallas as pl
from jax.experimental.pallas import tpu as pltpu
from jax.sharding import PartitionSpec as P

ROPE_THETA = 500000.0
EPS = 1e-5
NEG = -1e30
MESH = pl.DeviceIdType.MESH
F32 = jnp.float32
BF16 = jnp.bfloat16

B = 32
D = 3072
HD = 128
G = 4
R = 3
T = 256
HALF = D // 2
QC = 4
KC = 8
BC = B // KC
NC = 3
CW = HALF // NC
FF = 1024
SCALE = HD ** -0.5


def rms(values, gain):
    inv = lax.rsqrt(jnp.mean(values * values, axis=-1, keepdims=True) + EPS)
    return (values * inv * gain).astype(BF16)


def layer_kernel(
    ctx, freq, x_hbm, ga_hbm, gm_hbm, wq_hbm, wo_hbm, wg_hbm, wu_hbm, wd_hbm, k_hbm, v_hbm,
    kpin, vpin, knew, vnew, xout,
    x, ga, gm, wq, wo, wg, wu, wd, nbuf, acc, ang, qkv, qbuf, snbuf, obuf, mbuf, lbuf, rows, msg, cbuf,
    part1, drecv1, sum1a, recv1a, sum1b, recv1b, hbuf,
    part2, drecv2, sum2a, recv2a, sum2b, recv2b, ybuf,
    in_sem, wq_sem, kv_sem, w_sem, q_send, q_recv, c_send, c_recv,
    d_send, d_recv, a_send, a_recv, b_send, b_recv, g_send, g_recv,
):
    tp = lax.axis_index("tp")
    kvp = lax.axis_index("kvp")
    core = lax.rem(kvp, 2)
    xpos = kvp // 2
    other = 1 - core
    partner = {"kvp": xpos * 2 + other}
    first = {"tp": lax.rem(tp + core, 2), "kvp": lax.rem(xpos + 1 - core, 2) * 2 + core}
    second = {"tp": lax.rem(tp + 1 - core, 2), "kvp": lax.rem(xpos + core, 2) * 2 + core}

    def start(src, dst, sem):
        copy = pltpu.make_async_copy(src, dst, sem)
        copy.start()
        return copy

    x_in = start(x_hbm, x, in_sem.at[0])
    ga_in = start(ga_hbm, ga, in_sem.at[1])
    gm_in = start(gm_hbm, gm, in_sem.at[2])
    qrows = D // QC
    for i in range(QC):
        start(wq_hbm.at[pl.ds(i * qrows, qrows), pl.ds(pl.multiple_of(core * 1280, 128), 1280)], wq.at[i], wq_sem.at[i])
    for i in range(KC):
        start(k_hbm.at[pl.ds(i * BC, BC)], kpin.at[pl.ds(i * BC, BC)], kv_sem.at[0, i])
        start(v_hbm.at[pl.ds(i * BC, BC)], vpin.at[pl.ds(i * BC, BC)], kv_sem.at[1, i])
    wo_in = [start(wo_hbm.at[:, pl.ds(i * HALF, HALF)], wo.at[i], w_sem.at[i]) for i in range(2)]
    wg_in = start(wg_hbm, wg, w_sem.at[2])
    wu_in = start(wu_hbm, wu, w_sem.at[3])
    wd_in = [start(wd_hbm.at[:, pl.ds(i * HALF, HALF)], wd.at[i], w_sem.at[4 + i]) for i in range(2)]

    barrier = pltpu.get_barrier_semaphore()
    for step in range(1, 4):
        pl.semaphore_signal(barrier, inc=1, device_id={"kvp": lax.rem(kvp + step, 4)}, device_id_type=MESH)
    pl.semaphore_signal(barrier, inc=1, device_id={"tp": 1 - tp}, device_id_type=MESH)

    for b in range(B):
        ang[pl.ds(b, 1), :] = jnp.full((1, HD), ctx[b], jnp.int32).astype(F32) * freq[...]
    cos_t = jnp.cos(ang[...])
    lane = lax.broadcasted_iota(jnp.int32, (B, HD), 1)
    sin_t = jnp.sin(ang[...]) * jnp.where(lane < HD // 2, -1.0, 1.0)

    x_in.wait()
    ga_in.wait()
    gm_in.wait()
    nbuf[...] = rms(x[...].astype(F32), ga[...].astype(F32))

    for i in range(QC):
        pltpu.make_async_copy(wq.at[i], wq.at[i], wq_sem.at[i]).wait()
        term = jnp.dot(nbuf[:, i * qrows:(i + 1) * qrows], wq[i], preferred_element_type=F32)
        acc[...] = term if i == 0 else acc[...] + term

    def rope(values):
        return values * cos_t + pltpu.roll(values, HD // 2, 1) * sin_t

    for j in range(2):
        for r in range(R + 2):
            col = (j * (R + 2) + r) * HD
            value = acc[:, col:col + HD]
            if r <= R:
                value = rope(value)
            qkv[core, j * (R + 2) + r] = value.astype(BF16).astype(F32)

    pl.semaphore_wait(barrier, 4)
    swap = pltpu.make_async_remote_copy(
        qkv.at[core], qkv.at[core], q_send, q_recv, device_id=partner, device_id_type=MESH)
    swap.start()
    swap.wait()

    first_pos = kvp * T
    row_of = lax.broadcasted_iota(jnp.int32, (B, HD), 0)
    ctx_rows = ang
    for b in range(B):
        ctx_rows[pl.ds(b, 1), :] = jnp.full((1, HD), ctx[b] - first_pos, jnp.int32).astype(F32)
    here = (ctx_rows[...] >= 0.0) & (ctx_rows[...] < float(T))
    for g in range(G):
        base = (g % 2) * (R + 2)
        key = qkv[g // 2, base + R]
        value = qkv[g // 2, base + R + 1]
        rows[0, pl.ds(g, B, stride=G), :] = key
        rows[1, pl.ds(g, B, stride=G), :] = value
        for r in range(R):
            query = qkv[g // 2, base + r]
            qbuf[pl.ds(G * g + r, B, stride=16), :] = query
            score = jnp.sum(query * key, axis=-1, keepdims=True) * SCALE
            snbuf[pl.ds(G * g + r, B, stride=16), :] = jnp.where(here, jnp.broadcast_to(score, (B, HD)), NEG)
        qbuf[pl.ds(G * g + R, B, stride=16), :] = jnp.zeros((B, HD), F32)
        snbuf[pl.ds(G * g + R, B, stride=16), :] = jnp.full((B, HD), NEG, F32)
    knew[...] = rows[0].astype(BF16)
    vnew[...] = rows[1].astype(BF16)

    wide = (32, T * G)
    col_i = lax.broadcasted_iota(jnp.int32, wide, 1)
    row_i = lax.broadcasted_iota(jnp.int32, wide, 0)
    same_head = lax.rem(col_i, G) == lax.rem(row_i // G, G)
    row_c = lax.broadcasted_iota(jnp.int32, (32, 1), 0)

    def attend(b0):
        def pick(ref, b):
            return ref[pl.ds(pl.multiple_of(b * 16, 16), 16), :]

        q0 = pick(qbuf, b0).astype(BF16)
        q1 = pick(qbuf, b0 + 1).astype(BF16)
        zero = jnp.zeros((16, HD), BF16)
        q = jnp.concatenate(
            [jnp.concatenate([q0, zero], axis=1), jnp.concatenate([zero, q1], axis=1)], axis=0)
        k = jnp.concatenate([kpin[b0], kpin[b0 + 1]], axis=1)
        s = lax.dot_general(q, k, (((1,), (1,)), ((), ())), preferred_element_type=F32) * SCALE
        limit = jnp.where(row_c < 16, (ctx[b0] - first_pos) * G, (ctx[b0 + 1] - first_pos) * G)
        valid = same_head & (col_i < limit)
        s = jnp.where(valid, s, NEG)
        sn = jnp.concatenate([pick(snbuf, b0), pick(snbuf, b0 + 1)], axis=0)[:, :1]
        top = jnp.maximum(jnp.max(s, axis=-1, keepdims=True), sn)
        w = jnp.where(valid, jnp.exp(s - top), 0.0)
        total = jnp.sum(w, axis=-1, keepdims=True)
        v = jnp.concatenate([vpin[b0], vpin[b0 + 1]], axis=1)
        o = jnp.dot(w.astype(BF16), v, preferred_element_type=F32)
        at0 = pl.ds(pl.multiple_of(b0 * 16, 16), 16)
        at1 = pl.ds(pl.multiple_of(b0 * 16 + 16, 16), 16)
        obuf[at0, :] = o[:16, :HD]
        obuf[at1, :] = o[16:, HD:]
        both = pl.ds(pl.multiple_of(b0 * 16, 32), 32)
        mbuf[both, :] = jnp.broadcast_to(top, (32, HD))
        lbuf[both, :] = jnp.broadcast_to(total, (32, HD))

    @pl.loop(0, KC)
    def _(i):
        part = pl.ds(i * BC, BC)
        pltpu.make_async_copy(k_hbm.at[part], kpin.at[part], kv_sem.at[0, i]).wait()
        pltpu.make_async_copy(v_hbm.at[part], vpin.at[part], kv_sem.at[1, i]).wait()
        for j in range(BC // 2):
            attend(i * BC + 2 * j)

    for g in range(G):
        value = qkv[g // 2, (g % 2) * (R + 2) + R + 1]
        stats = jnp.zeros((B, HD), F32)
        for r in range(R):
            at = pl.ds(G * g + r, B, stride=16)
            top = mbuf[at, :]
            fresh = jnp.where(here, jnp.exp(snbuf[at, :] - top), 0.0)
            msg[g, r] = obuf[at, :] + fresh.astype(BF16).astype(F32) * value
            stats = jnp.where(lane == r, top, jnp.where(lane == R + r, lbuf[at, :] + fresh, stats))
        msg[g, R] = stats
    sends = []
    for step in (2, 3, 1):
        peer = lax.rem(kvp + step, 4)
        copy = pltpu.make_async_remote_copy(
            msg.at[peer], cbuf.at[step], c_send.at[step], c_recv.at[step],
            device_id={"kvp": peer}, device_id_type=MESH)
        copy.start()
        sends.append(copy)
    cbuf[0] = msg[kvp]
    for copy in sends:
        copy.wait()

    heads = []
    slots = [lax.rem(kvp - p + 4, 4) for p in range(4)]
    stats = [cbuf[s, R] for s in slots]
    for r in range(R):
        tops = [st[:, r:r + 1] for st in stats]
        top = jnp.maximum(jnp.maximum(tops[0], tops[1]), jnp.maximum(tops[2], tops[3]))
        num, den = None, None
        for s, st, t in zip(slots, stats, tops):
            f = jnp.exp(t - top)
            n_term, d_term = cbuf[s, r] * f, st[:, R + r:R + r + 1] * f
            num = n_term if num is None else num + n_term
            den = d_term if den is None else den + d_term
        heads.append((num / den).astype(BF16))
    attn = jnp.concatenate(heads, axis=1)

    def remote(src, dst, send, recv, peer):
        copy = pltpu.make_async_remote_copy(src, dst, send, recv, device_id=peer, device_id_type=MESH)
        copy.start()
        return copy

    def reduce(k, lhs, weight, part, drecv, suma, recva, sumb, recvb, out, finish):
        pend = []
        for c in range(NC):
            part[c] = jnp.dot(lhs, weight[other, :, c * CW:(c + 1) * CW], preferred_element_type=F32)
            pend.append(remote(part.at[c], drecv.at[c], d_send.at[k, c], d_recv.at[k, c], partner))
        own = [jnp.dot(lhs, weight[core, :, c * CW:(c + 1) * CW], preferred_element_type=F32) for c in range(NC)]
        last = pend
        pend = []
        for c in range(NC):
            last[c].wait()
            suma[c] = own[c] + drecv[c]
            pend.append(remote(suma.at[c], recva.at[c], a_send.at[k, c], a_recv.at[k, c], first))
        last = pend
        pend = []
        for c in range(NC):
            last[c].wait()
            sumb[c] = suma[c] + recva[c]
            pend.append(remote(sumb.at[c], recvb.at[c], b_send.at[k, c], b_recv.at[k, c], second))
        last = pend
        pend = []
        for c in range(NC):
            last[c].wait()
            out[core, c] = finish(c, sumb[c] + recvb[c])
            pend.append(remote(out.at[core, c], out.at[core, c], g_send.at[k, c], g_recv.at[k, c], partner))
        for copy in pend:
            copy.wait()

    def half_of(ref, c):
        return ref[:, pl.ds(pl.multiple_of(core * HALF + c * CW, 128), CW)]

    for copy in wo_in:
        copy.wait()
    reduce(0, attn, wo, part1, drecv1, sum1a, recv1a, sum1b, recv1b, hbuf,
           lambda c, total: (half_of(x, c).astype(F32) + total).astype(BF16).astype(F32))

    square = jnp.zeros((B, 1), F32)
    for i in range(2):
        for c in range(NC):
            square = square + jnp.sum(hbuf[i, c] * hbuf[i, c], axis=-1, keepdims=True)
    inv = lax.rsqrt(square * (1.0 / D) + EPS)
    for i in range(2):
        for c in range(NC):
            col = i * HALF + c * CW
            nbuf[:, col:col + CW] = (hbuf[i, c] * inv * gm[:, col:col + CW].astype(F32)).astype(BF16)
    wg_in.wait()
    wu_in.wait()
    acts = []
    for c in range(FF // 256):
        cols = slice(c * 256, (c + 1) * 256)
        gate = jnp.dot(nbuf[...], wg[:, cols], preferred_element_type=F32)
        up = jnp.dot(nbuf[...], wu[:, cols], preferred_element_type=F32)
        acts.append((gate * (1.0 / (1.0 + jnp.exp(-gate))) * up).astype(BF16))
    act = jnp.concatenate(acts, axis=1)
    for copy in wd_in:
        copy.wait()
    reduce(1, act, wd, part2, drecv2, sum2a, recv2a, sum2b, recv2b, ybuf,
           lambda c, total: (hbuf[core, c] + total).astype(BF16).astype(F32))
    for i in range(2):
        for c in range(NC):
            col = i * HALF + c * CW
            xout[:, col:col + CW] = ybuf[i, c].astype(BF16)


def write_kernel(ctx, k, v, knew, vnew, x, ko, vo, y, sem, row_sem):
    first_pos = lax.axis_index("kvp") * T
    pairs = ((k, knew, ko), (v, vnew, vo))

    def bulk(n, i):
        part = pl.ds(i * BC, BC)
        return pltpu.make_async_copy(pairs[n][0].at[part], pairs[n][2].at[part], sem.at[n, i])

    def row(n, b):
        pos = jnp.clip(ctx[b] - first_pos, 0, T - 1)
        return pltpu.make_async_copy(pairs[n][1].at[b], pairs[n][2].at[b, pos], row_sem)

    def held(b):
        pos = ctx[b] - first_pos
        return (pos >= 0) & (pos < T)

    x_copy = pltpu.make_async_copy(x, y, sem.at[2, 0])
    x_copy.start()
    for i in range(KC):
        for n in range(2):
            bulk(n, i).start()

    @pl.loop(0, KC)
    def _(i):
        for n in range(2):
            bulk(n, i).wait()

            @pl.loop(0, BC)
            def _(j):
                b = i * BC + j

                @pl.when(held(b))
                def _():
                    row(n, b).start()

    @pl.loop(0, B)
    def _(b):
        @pl.when(held(b))
        def _():
            row(0, b).wait()
            row(1, b).wait()

    x_copy.wait()


def solution(mesh):
    x_spec = P("dp", None)
    cache_spec = P("dp", "kvp", "tp", None)
    model_axes = ("tp", "kvp")
    inv_freq = (ROPE_THETA ** (-2.0 * np.arange(HD // 2) / HD)).astype(np.float32)
    freq = np.concatenate([inv_freq, inv_freq])[None]

    def layer_step(x_in, ctx_len, g_attn, g_mlp, w_qkv, w_o, w_gate, w_up, w_down, k_cache, v_cache):
        hbm = functools.partial(pltpu.with_memory_space_constraint, memory_space=pltpu.HBM)
        vmem = pl.BlockSpec(memory_space=pltpu.VMEM)
        anyspace = pl.BlockSpec(memory_space=pltpu.HBM)
        smem = pl.BlockSpec(memory_space=pltpu.SMEM)
        flat = (B, T * G, HD)
        chunk = pltpu.VMEM((NC, B, CW), F32)
        dma = pltpu.SemaphoreType.DMA
        kpin, vpin, knew, vnew, x_out = pl.pallas_call(
            layer_kernel,
            name="layer",
            out_shape=(
                pltpu.VMEM(flat, BF16),
                pltpu.VMEM(flat, BF16),
                pltpu.VMEM((B * G, HD), BF16),
                pltpu.VMEM((B * G, HD), BF16),
                pltpu.VMEM((B, D), BF16),
            ),
            in_specs=[smem, vmem] + [anyspace] * 10,
            out_specs=(vmem,) * 5,
            scratch_shapes=[
                pltpu.VMEM((B, D), BF16),
                pltpu.VMEM((1, D), BF16),
                pltpu.VMEM((1, D), BF16),
                pltpu.VMEM((QC, D // QC, 1280), BF16),
                pltpu.VMEM((2, 384, HALF), BF16),
                pltpu.VMEM((D, FF), BF16),
                pltpu.VMEM((D, FF), BF16),
                pltpu.VMEM((2, FF, HALF), BF16),
                pltpu.VMEM((B, D), BF16),
                pltpu.VMEM((B, 1280), F32),
                pltpu.VMEM((B, HD), F32),
                pltpu.VMEM((2, 10, B, HD), F32),
                pltpu.VMEM((B * 16, HD), F32),
                pltpu.VMEM((B * 16, HD), F32),
                pltpu.VMEM((B * 16, HD), F32),
                pltpu.VMEM((B * 16, HD), F32),
                pltpu.VMEM((B * 16, HD), F32),
                pltpu.VMEM((2, B * G, HD), F32),
                pltpu.VMEM((G, R + 1, B, HD), F32),
                pltpu.VMEM((4, R + 1, B, HD), F32),
            ]
            + ([chunk] * 6 + [pltpu.VMEM((2, NC, B, CW), F32)]) * 2
            + [dma((3,)), dma((QC,)), dma((2, KC)), dma((6,)), dma, dma, dma((4,)), dma((4,))]
            + [dma((2, NC))] * 8,
            compiler_params=pltpu.CompilerParams(
                collective_id=0, has_side_effects=True, vmem_limit_bytes=38 * 2 ** 20),
        )(
            ctx_len, freq, hbm(x_in), hbm(g_attn.reshape(1, D)), hbm(g_mlp.reshape(1, D)), hbm(w_qkv), hbm(w_o),
            hbm(w_gate), hbm(w_up), hbm(w_down), hbm(k_cache.reshape(flat)), hbm(v_cache.reshape(flat)))
        k_out, v_out, x_out = pl.pallas_call(
            write_kernel,
            name="write",
            out_shape=(
                jax.ShapeDtypeStruct(k_cache.shape, BF16),
                jax.ShapeDtypeStruct(v_cache.shape, BF16),
                jax.ShapeDtypeStruct(x_in.shape, BF16),
            ),
            in_specs=[smem] + [vmem] * 5,
            out_specs=(anyspace,) * 3,
            scratch_shapes=[dma((3, KC)), dma],
            compiler_params=pltpu.CompilerParams(vmem_limit_bytes=2 ** 20),
        )(
            ctx_len, kpin.reshape(k_cache.shape), vpin.reshape(v_cache.shape),
            knew.reshape(B, G, HD), vnew.reshape(B, G, HD), x_out)
        return x_out, k_out, v_out

    in_specs = (
        x_spec, P("dp"), P(None), P(None), P(None, "tp"), P(model_axes, None), P(None, model_axes),
        P(None, model_axes), P(model_axes, None), cache_spec, cache_spec)
    return jax.shard_map(
        layer_step, mesh=mesh, in_specs=in_specs, out_specs=(x_spec, cache_spec, cache_spec), check_vma=False)
```

```python
import functools

import jax
import jax.numpy as jnp
import numpy as np
from jax import lax
from jax.experimental import pallas as pl
from jax.experimental.pallas import tpu as pltpu
from jax.sharding import PartitionSpec as P


ROPE_THETA = 500000.0
EPS = 1e-5
NEG = -1e30
MESH = pl.DeviceIdType.MESH
F32 = jnp.float32
BF16 = jnp.bfloat16

B = 32
D = 3072
HD = 128
G = 4
R = 3
T = 256
HALF = D // 2
QC = 4
KC = 8
BC = B // KC
NC = 3
CW = HALF // NC
FF = 1024
SCALE = HD ** -0.5 * np.log2(np.e)


def rms(values, gain):
    inv = lax.rsqrt(jnp.mean(values * values, axis=-1, keepdims=True) + EPS)
    return (values * inv * gain).astype(BF16)


def layer_kernel(
    ctx_hbm, freq_hbm, x_hbm, ga_hbm, gm_hbm, wq_hbm, wo_hbm, wg_hbm, wu_hbm, wd_hbm, k_hbm, v_hbm,
    kpin, vpin, knew, vnew, xout,
    ctx, freq, x, ga, gm, wq, wo, wg, wu, wd, nbuf, acc, rel, qkv, qbuf, snbuf, colp, sbuf, wbuf, obuf, mbuf, lbuf,
    rows, msg, cbuf,
    part1, drecv1, sum1a, recv1a, sum1b, recv1b, hbuf,
    part2, drecv2, sum2a, recv2a, sum2b, recv2b, ybuf,
    in_sem, wq_sem, kv_sem, w_sem, q_send, q_recv, c_send, c_recv,
    d_send, d_recv, a_send, a_recv, b_send, b_recv, g_send, g_recv,
):
    open_scope = []

    def phase(name):
        if open_scope:
            open_scope.pop().__exit__(None, None, None)
        if name:
            open_scope.append(jax.named_scope(name))
            open_scope[0].__enter__()

    tp = lax.axis_index("tp")
    kvp = lax.axis_index("kvp")
    core = lax.rem(kvp, 2)
    xpos = kvp // 2
    other = 1 - core
    partner = {"kvp": xpos * 2 + other}
    first = {"tp": lax.rem(tp + core, 2), "kvp": lax.rem(xpos + 1 - core, 2) * 2 + core}
    second = {"tp": lax.rem(tp + 1 - core, 2), "kvp": lax.rem(xpos + core, 2) * 2 + core}

    def start(src, dst, sem):
        copy = pltpu.make_async_copy(src, dst, sem)
        copy.start()
        return copy

    x_in = start(x_hbm, x, in_sem.at[0])
    ctx_in = start(ctx_hbm, ctx, in_sem.at[3])
    freq_in = start(freq_hbm, freq, in_sem.at[4])
    ga_in = start(ga_hbm, ga, in_sem.at[1])
    gm_in = start(gm_hbm, gm, in_sem.at[2])
    qrows = D // QC
    wq_in = [
        start(wq_hbm.at[pl.ds(i * qrows, qrows), pl.ds(pl.multiple_of(core * 1280, 128), 1280)], wq.at[i], wq_sem.at[i])
        for i in range(QC)
    ]

    def cache(n, i):
        part = pl.ds(i * BC, BC)
        src, dst = ((k_hbm, kpin), (v_hbm, vpin))[n]
        return pltpu.make_async_copy(src.at[part], dst.at[part], kv_sem.at[n, i])

    order = [(0, 0), (0, 1)]
    for i in range(KC - 2):
        order += [(1, i), (0, i + 2)]
    order += [(1, KC - 2), (1, KC - 1)]

    def read_caches(first, last):
        for n, i in order[first:last]:
            cache(n, i).start()

    wo_in = [pltpu.make_async_copy(wo_hbm.at[:, pl.ds(i * HALF, HALF)], wo.at[i], w_sem.at[i]) for i in range(2)]
    wg_in = pltpu.make_async_copy(wg_hbm, wg, w_sem.at[2])
    wu_in = pltpu.make_async_copy(wu_hbm, wu, w_sem.at[3])
    wd_in = [pltpu.make_async_copy(wd_hbm.at[:, pl.ds(i * HALF, HALF)], wd.at[i], w_sem.at[4 + i]) for i in range(2)]

    barrier = pltpu.get_barrier_semaphore()
    for step in range(1, 4):
        pl.semaphore_signal(barrier, inc=1, device_id={"kvp": lax.rem(kvp + step, 4)}, device_id_type=MESH)
    pl.semaphore_signal(barrier, inc=1, device_id={"tp": 1 - tp}, device_id_type=MESH)

    phase("tables")
    first_pos = kvp * T
    ctx_in.wait()
    freq_in.wait()
    lane = lax.broadcasted_iota(jnp.int32, (B, HD), 1)
    own_lane = lax.broadcasted_iota(jnp.int32, (B, B), 0) == lax.broadcasted_iota(jnp.int32, (B, B), 1)
    ctx_col = jnp.sum(jnp.where(own_lane, ctx[...].astype(F32)[None, :], 0.0), axis=1, keepdims=True)
    pos_b = jnp.broadcast_to(ctx_col, (B, HD))
    rel[...] = pos_b - (first_pos * 1.0)
    angle = pos_b * freq[...]
    cos_t = jnp.cos(angle)
    sin_t = jnp.sin(angle) * jnp.where(lane < HD // 2, -1.0, 1.0)

    phase("norm")
    x_in.wait()
    ga_in.wait()
    gm_in.wait()
    nbuf[...] = rms(x[...].astype(F32), ga[...].astype(F32)[None, :])

    phase("qkv")
    for i in range(QC):
        wq_in[i].wait()
        read_caches(2 * i, 2 * i + 2)
        term = jnp.dot(nbuf[:, i * qrows:(i + 1) * qrows], wq[i], preferred_element_type=F32)
        acc[...] = term if i == 0 else acc[...] + term

    phase("rope")
    def rope(values):
        return values * cos_t + pltpu.roll(values, HD // 2, 1) * sin_t

    for j in range(2):
        for r in range(R + 2):
            col = (j * (R + 2) + r) * HD
            value = acc[:, col:col + HD]
            if r <= R:
                value = rope(value)
            qkv[core, j * (R + 2) + r] = value.astype(BF16).astype(F32)

    phase("swap")
    pl.semaphore_wait(barrier, 4)
    swap = pltpu.make_async_remote_copy(
        qkv.at[core], qkv.at[core], q_send, q_recv, device_id=partner, device_id_type=MESH)
    swap.start()
    read_caches(2 * QC, 2 * QC + 2)
    swap.wait()

    phase("qrows")
    here = (rel[...] >= 0.0) & (rel[...] < float(T))
    for g in range(G):
        base = (g % 2) * (R + 2)
        key = qkv[g // 2, base + R]
        value = qkv[g // 2, base + R + 1]
        rows[0, pl.ds(g, B, stride=G), :] = key
        rows[1, pl.ds(g, B, stride=G), :] = value
        for r in range(R):
            query = qkv[g // 2, base + r]
            qbuf[pl.ds(G * g + r, B, stride=16), :] = query
            score = jnp.sum(query * key, axis=-1, keepdims=True) * SCALE
            snbuf[pl.ds(G * g + r, B, stride=16), :] = jnp.where(here, jnp.broadcast_to(score, (B, HD)), NEG)
        qbuf[pl.ds(G * g + R, B, stride=16), :] = jnp.zeros((B, HD), F32)
        snbuf[pl.ds(G * g + R, B, stride=16), :] = jnp.full((B, HD), NEG, F32)
    knew[...] = rows[0].astype(BF16)
    vnew[...] = rows[1].astype(BF16)

    col_i = lax.broadcasted_iota(jnp.int32, (16, T * G), 1)
    row_i = lax.broadcasted_iota(jnp.int32, (16, T * G), 0)
    colp[...] = jnp.where(lax.rem(col_i, G) == row_i // G, (col_i // G).astype(F32), 1e9)
    lane8 = lax.broadcasted_iota(jnp.int32, (8, HD), 1)

    def rows16(b):
        return pl.ds(pl.multiple_of(b * 16, 16), 16)

    def scores(i):
        for j in range(BC // 2):
            b = i * BC + 2 * j
            q0 = qbuf[rows16(b), :].astype(BF16)
            q1 = qbuf[rows16(b + 1), :].astype(BF16)
            zero = jnp.zeros((16, HD), BF16)
            q = jnp.concatenate(
                [jnp.concatenate([q0, zero], axis=1), jnp.concatenate([zero, q1], axis=1)], axis=0)
            k = jnp.concatenate([kpin[b], kpin[b + 1]], axis=1)
            sbuf[j] = lax.dot_general(q, k, (((1,), (1,)), ((), ())), preferred_element_type=F32)

    def weights(i):
        for j in range(BC):
            b = i * BC + j
            half = slice(16 * (j % 2), 16 * (j % 2) + 16)
            limit = jnp.broadcast_to(rel[pl.ds(b, 1), :], (16, HD))
            valid = colp[...] < jnp.concatenate([limit] * (T * G // HD), axis=1)
            s = jnp.where(valid, sbuf[j // 2, half, :] * SCALE, NEG)
            top = jnp.maximum(jnp.max(s, axis=-1, keepdims=True), snbuf[rows16(b), :1])
            w = jnp.where(valid, jnp.exp2(s - top), 0.0)
            wbuf[j // 2, half, :] = w.astype(BF16)
            mbuf[rows16(b), :] = jnp.broadcast_to(top, (16, HD))
            lbuf[rows16(b), :] = jnp.broadcast_to(jnp.sum(w, axis=-1, keepdims=True), (16, HD))

    def values(i):
        for j in range(BC // 2):
            b = i * BC + 2 * j
            v = jnp.concatenate([vpin[b], vpin[b + 1]], axis=1)
            o = jnp.dot(wbuf[j], v, preferred_element_type=F32)
            obuf[rows16(b), :] = o[:16, :HD]
            obuf[rows16(b + 1), :] = o[16:, HD:]

    def message(step, c):
        peer = lax.rem(kvp + step, 4)
        return pltpu.make_async_remote_copy(
            msg.at[c, peer], cbuf.at[step, c], c_send.at[step, c], c_recv.at[step, c],
            device_id={"kvp": peer}, device_id_type=MESH)

    def emit(c):
        part = pl.ds(pl.multiple_of(c * 8, 8), 8)
        near = (rel[part, :] >= 0.0) & (rel[part, :] < float(T))
        for g in range(G):
            value = qkv[g // 2, (g % 2) * (R + 2) + R + 1, part, :]
            stats = jnp.zeros((8, HD), F32)
            for r in range(R):
                at = pl.ds(c * 128 + G * g + r, 8, stride=16)
                top = mbuf[at, :]
                fresh = jnp.where(near, jnp.exp2(snbuf[at, :] - top), 0.0)
                msg[c, g, r] = obuf[at, :] + fresh.astype(BF16).astype(F32) * value
                stats = jnp.where(lane8 == r, top, jnp.where(lane8 == R + r, lbuf[at, :] + fresh, stats))
            msg[c, g, R] = stats
        for step in (2, 3, 1):
            message(step, c).start()
        cbuf[0, c] = msg[c, kvp]

    phase("attn_head")
    cache(0, 0).wait()
    scores(0)
    read_caches(2 * QC + 2, 2 * QC + 4)
    cache(0, 1).wait()
    weights(0)
    scores(1)
    read_caches(2 * QC + 4, 2 * KC)

    phase("attn_loop")
    @pl.loop(2, KC)
    def _(i):
        for n, c in ((0, i), (1, i - 2)):
            cache(n, c).wait()
        values(i - 2)
        weights(i - 1)
        scores(i)

        for at, copies in ((3, wo_in), (4, [wg_in]), (5, [wu_in]), (6, wd_in)):
            @pl.when(i == at)
            def _():
                for copy in copies:
                    copy.start()

        @pl.when(lax.rem(i, 2) == 1)
        def _():
            emit((i - 3) // 2)

    phase("attn_tail")
    cache(1, KC - 2).wait()
    values(KC - 2)
    weights(KC - 1)
    cache(1, KC - 1).wait()
    values(KC - 1)
    emit(3)
    phase("msg_wait")
    for c in range(4):
        for step in (2, 3, 1):
            message(step, c).wait()

    phase("combine")
    heads = []
    slots = [lax.rem(kvp - p + 4, 4) for p in range(4)]
    stats = [cbuf[s, :, R].reshape(B, HD) for s in slots]
    for r in range(R):
        tops = [st[:, r:r + 1] for st in stats]
        top = jnp.maximum(jnp.maximum(tops[0], tops[1]), jnp.maximum(tops[2], tops[3]))
        num, den = None, None
        for s, st, t in zip(slots, stats, tops):
            f = jnp.exp2(t - top)
            n_term, d_term = cbuf[s, :, r].reshape(B, HD) * f, st[:, R + r:R + r + 1] * f
            num = n_term if num is None else num + n_term
            den = d_term if den is None else den + d_term
        heads.append((num / den).astype(BF16))
    attn = jnp.concatenate(heads, axis=1)

    def remote(src, dst, send, recv, peer):
        copy = pltpu.make_async_remote_copy(src, dst, send, recv, device_id=peer, device_id_type=MESH)
        copy.start()
        return copy

    def reduce(k, lhs, weight, part, drecv, suma, recva, sumb, recvb, out, finish):
        phase(f"part{k}")
        pend = []
        for c in range(NC):
            part[c] = jnp.dot(lhs, weight[other, :, c * CW:(c + 1) * CW], preferred_element_type=F32)
            pend.append(remote(part.at[c], drecv.at[c], d_send.at[k, c], d_recv.at[k, c], partner))
        own = [jnp.dot(lhs, weight[core, :, c * CW:(c + 1) * CW], preferred_element_type=F32) for c in range(NC)]
        phase(f"chip{k}")
        last = pend
        pend = []
        for c in range(NC):
            last[c].wait()
            suma[c] = own[c] + drecv[c]
            pend.append(remote(suma.at[c], recva.at[c], a_send.at[k, c], a_recv.at[k, c], first))
        phase(f"first{k}")
        last = pend
        pend = []
        for c in range(NC):
            last[c].wait()
            sumb[c] = suma[c] + recva[c]
            pend.append(remote(sumb.at[c], recvb.at[c], b_send.at[k, c], b_recv.at[k, c], second))
        phase(f"second{k}")
        last = pend
        pend = []
        for c in range(NC):
            last[c].wait()
            out[core, c] = finish(c, sumb[c] + recvb[c])
            pend.append(remote(out.at[core, c], out.at[core, c], g_send.at[k, c], g_recv.at[k, c], partner))
        phase(f"gather{k}")
        for copy in pend:
            copy.wait()

    def half_of(ref, c):
        return ref[:, pl.ds(pl.multiple_of(core * HALF + c * CW, 128), CW)]

    phase("wo_wait")
    for copy in wo_in:
        copy.wait()
    reduce(0, attn, wo, part1, drecv1, sum1a, recv1a, sum1b, recv1b, hbuf,
           lambda c, total: (half_of(x, c).astype(F32) + total).astype(BF16).astype(F32))

    phase("mlp_norm")
    square = jnp.zeros((B, 1), F32)
    for i in range(2):
        for c in range(NC):
            square = square + jnp.sum(hbuf[i, c] * hbuf[i, c], axis=-1, keepdims=True)
    inv = lax.rsqrt(square * (1.0 / D) + EPS)
    for i in range(2):
        for c in range(NC):
            col = i * HALF + c * CW
            nbuf[:, col:col + CW] = (hbuf[i, c] * inv * gm[pl.ds(col, CW)].astype(F32)[None, :]).astype(BF16)
    phase("gate_up")
    wg_in.wait()
    wu_in.wait()
    acts = []
    for c in range(FF // 256):
        cols = slice(c * 256, (c + 1) * 256)
        gate = jnp.dot(nbuf[...], wg[:, cols], preferred_element_type=F32)
        up = jnp.dot(nbuf[...], wu[:, cols], preferred_element_type=F32)
        acts.append((gate * (1.0 / (1.0 + jnp.exp(-gate))) * up).astype(BF16))
    act = jnp.concatenate(acts, axis=1)
    phase("wd_wait")
    for copy in wd_in:
        copy.wait()
    reduce(1, act, wd, part2, drecv2, sum2a, recv2a, sum2b, recv2b, ybuf,
           lambda c, total: (hbuf[core, c] + total).astype(BF16).astype(F32))
    phase("out")
    for i in range(2):
        for c in range(NC):
            col = i * HALF + c * CW
            xout[:, col:col + CW] = ybuf[i, c].astype(BF16)
    phase(None)


def write_kernel(ctx, k, v, knew, vnew, x, ko, vo, y, sem, row_sem):
    first_pos = lax.axis_index("kvp") * T
    pairs = ((k, knew, ko), (v, vnew, vo))

    def bulk(i):
        part = pl.ds(i * BC, BC)
        return [pltpu.make_async_copy(p[0].at[part], p[2].at[part], sem.at[n, i]) for n, p in enumerate(pairs)]

    def new_rows(b, act):
        pos = ctx[b] - first_pos

        @pl.when((pos >= 0) & (pos < T))
        def _():
            for n, p in enumerate(pairs):
                act(pltpu.make_async_copy(p[1].at[b], p[2].at[b, pos], row_sem.at[n]))

    x_copy = pltpu.make_async_copy(x, y, sem.at[2, 0])
    x_copy.start()
    ahead = 4
    for i in range(ahead):
        for copy in bulk(i):
            copy.start()
    for i in range(KC):
        for copy in bulk(i):
            copy.wait()
        if i + ahead < KC:
            for copy in bulk(i + ahead):
                copy.start()
        for j in range(BC):
            new_rows(i * BC + j, lambda copy: copy.start())

    @pl.loop(0, B)
    def _(b):
        new_rows(b, lambda copy: copy.wait())

    x_copy.wait()


def solution(mesh):
    x_spec = P("dp", None)
    cache_spec = P("dp", "kvp", "tp", None)
    model_axes = ("tp", "kvp")
    inv_freq = (ROPE_THETA ** (-2.0 * np.arange(HD // 2) / HD)).astype(np.float32)
    freq = jnp.asarray(np.concatenate([inv_freq, inv_freq])[None])

    def layer_step(x_in, ctx_len, g_attn, g_mlp, w_qkv, w_o, w_gate, w_up, w_down, k_cache, v_cache):
        hbm = functools.partial(pltpu.with_memory_space_constraint, memory_space=pltpu.HBM)
        vmem = pl.BlockSpec(memory_space=pltpu.VMEM)
        anyspace = pl.BlockSpec(memory_space=pltpu.HBM)
        smem = pl.BlockSpec(memory_space=pltpu.SMEM)
        flat = (B, T * G, HD)
        chunk = pltpu.VMEM((NC, B, CW), F32)
        dma = pltpu.SemaphoreType.DMA
        kpin, vpin, knew, vnew, x_out = pl.pallas_call(
            layer_kernel,
            name="layer",
            out_shape=(
                pltpu.VMEM(flat, BF16),
                pltpu.VMEM(flat, BF16),
                pltpu.VMEM((B * G, HD), BF16),
                pltpu.VMEM((B * G, HD), BF16),
                pltpu.VMEM((B, D), BF16),
            ),
            in_specs=[anyspace] * 12,
            out_specs=(vmem,) * 5,
            scratch_shapes=[
                pltpu.VMEM((B,), jnp.int32),
                pltpu.VMEM((1, HD), F32),
                pltpu.VMEM((B, D), BF16),
                pltpu.VMEM((D,), BF16),
                pltpu.VMEM((D,), BF16),
                pltpu.VMEM((QC, D // QC, 1280), BF16),
                pltpu.VMEM((2, 384, HALF), BF16),
                pltpu.VMEM((D, FF), BF16),
                pltpu.VMEM((D, FF), BF16),
                pltpu.VMEM((2, FF, HALF), BF16),
                pltpu.VMEM((B, D), BF16),
                pltpu.VMEM((B, 1280), F32),
                pltpu.VMEM((B, HD), F32),
                pltpu.VMEM((2, 10, B, HD), F32),
                pltpu.VMEM((B * 16, HD), F32),
                pltpu.VMEM((B * 16, HD), F32),
                pltpu.VMEM((16, T * G), F32),
                pltpu.VMEM((BC // 2, 32, T * G), F32),
                pltpu.VMEM((BC // 2, 32, T * G), BF16),
                pltpu.VMEM((B * 16, HD), F32),
                pltpu.VMEM((B * 16, HD), F32),
                pltpu.VMEM((B * 16, HD), F32),
                pltpu.VMEM((2, B * G, HD), F32),
                pltpu.VMEM((4, G, R + 1, 8, HD), F32),
                pltpu.VMEM((4, 4, R + 1, 8, HD), F32),
            ]
            + ([chunk] * 6 + [pltpu.VMEM((2, NC, B, CW), F32)]) * 2
            + [dma((5,)), dma((QC,)), dma((2, KC)), dma((6,)), dma, dma, dma((4, 4)), dma((4, 4))]
            + [dma((2, NC))] * 8,
            compiler_params=pltpu.CompilerParams(
                collective_id=0, has_side_effects=True, vmem_limit_bytes=38 * 2 ** 20),
        )(
            hbm(ctx_len), hbm(freq), hbm(x_in), hbm(g_attn), hbm(g_mlp), hbm(w_qkv), hbm(w_o),
            hbm(w_gate), hbm(w_up), hbm(w_down), hbm(k_cache.reshape(flat)), hbm(v_cache.reshape(flat)))
        k_out, v_out, x_out = pl.pallas_call(
            write_kernel,
            name="write",
            out_shape=(
                jax.ShapeDtypeStruct(k_cache.shape, BF16),
                jax.ShapeDtypeStruct(v_cache.shape, BF16),
                jax.ShapeDtypeStruct(x_in.shape, BF16),
            ),
            in_specs=[smem] + [vmem] * 5,
            out_specs=(anyspace,) * 3,
            scratch_shapes=[dma((3, KC)), dma((2,))],
            compiler_params=pltpu.CompilerParams(vmem_limit_bytes=2 ** 20),
        )(
            ctx_len, kpin.reshape(k_cache.shape), vpin.reshape(v_cache.shape),
            knew.reshape(B, G, HD), vnew.reshape(B, G, HD), x_out)
        return x_out, k_out, v_out

    in_specs = (
        x_spec, P("dp"), P(None), P(None), P(None, "tp"), P(model_axes, None), P(None, model_axes),
        P(None, model_axes), P(model_axes, None), cache_spec, cache_spec)
    return jax.shard_map(
        layer_step, mesh=mesh, in_specs=in_specs, out_specs=(x_spec, cache_spec, cache_spec), check_vma=False)
```
